256 devices in a mesh: blk: 4 (over z_lo), pts: 64 (over y, z_hi, x, core).
Axes of the slice: x: 4, y: 4, z: 8 (z_hi: 2, z_lo: 4; z = z_hi * 4 + z_lo), core: 2. Of those that a mesh axis runs over, the one named last changes fastest.
Arguments:
- signal: bfloat16 [67584, 16384], P('blk', 'pts'), may hold values from -6 to 6
- offsets: int32 [128], P('blk'), may hold values from 0 to 15872
- kept: int32 [128], replicated, may hold values from 0 to 512
- weights: float32 [16384], P('pts'), may hold values from 0.2 to 5
Outputs:
- gram: float32 [128, 2, 128, 128], P('pts', None, 'blk')
The draws below stay inside these ranges and needn't reach their ends.
Inputs may be any that keep to these rules, and one draw needn't show every extreme that they name: `kept`: indices may repeat.
All inputs are finite; a program needn't handle non-finite values.
Results may differ from the reference program's by a relative error of at most 0.0022.
Values may be sent and summed in bfloat16 or wider, within the bound.
A program may use at most 128 MiB of HBM per device.

```python
import math
import jax
import jax.numpy as jnp
from jax import lax

NFFT = 1024
BLK_DEV = 32
NB = 128
K = 128
POINTS = 16384
SEG = 16896
TIME = 67584


def place_ends(entries, own_key, low, top_value):
    shape = entries.shape
    place = [jax.random.randint(jax.random.fold_in(own_key, axis), (), 0, shape[axis]) for axis in range(len(shape))]
    entries = entries.at[tuple(place)].set(low)
    longest = shape.index(max(shape))
    place[longest] = (place[longest] + 1) % shape[longest]
    return entries.at[tuple(place)].set(top_value)


def block_scale(rng, shape, split, smallest, high):
    gain = 1.0
    for position, blocks in split:
        steps = jax.random.uniform(jax.random.fold_in(jax.random.fold_in(rng, 6), position), (blocks,), jnp.float32, smallest / len(split), high / len(split))
        gain = gain * jnp.repeat(jnp.exp(steps), shape[position] // blocks).reshape((-1,) + (1,) * (len(shape) - 1 - position))
    return gain


def normal_values(key, dims, scale, bound, split=(), kind=jnp.bfloat16):
    loudness = block_scale(key, dims, split, -0.22, 0.18) if split else 1.0
    entries = jax.random.normal(key, dims, jnp.float32) * scale * loudness
    return jnp.minimum(jnp.maximum(entries, -bound), bound).astype(kind)


def setup_inputs(seed: int = 0) -> dict:
    key_list = jax.random.split(jax.random.key(seed), 5)
    signal = normal_values(key_list[0], (TIME, POINTS), 1.0, 6.0, ((0, 4), (1, 64)))
    offsets = place_ends(jax.random.randint(key_list[1], (NB,), 0, SEG - NFFT + 1), jax.random.fold_in(key_list[1], 1), 0, SEG - NFFT).astype(jnp.int32)
    kept = place_ends(jax.random.randint(key_list[2], (K,), 0, NFFT // 2 + 1), jax.random.fold_in(key_list[2], 1), 0, (NFFT // 2 + 1) - 1).astype(jnp.int32)
    weights = jnp.clip(jnp.exp(math.log(5.0) - 3.218876 * jax.random.uniform(key_list[3], (POINTS,), jnp.float32) ** block_scale(key_list[3], (POINTS,), ((0, 64),), -0.2, 0.2)), 0.2, 5.0)
    return dict(signal=signal, offsets=offsets, kept=kept, weights=weights)


def spectral_table(kept, length):
    times = jnp.arange(length, dtype=jnp.int32)
    window = 0.5 - 0.5 * jnp.cos(times.astype(jnp.float32) * (2.0 * math.pi / length))
    norm = 1.0 / jnp.sqrt(jnp.sum(window * window))
    phase_index = times[:, None] * kept[None, :].astype(jnp.int32) % length
    phase = phase_index.astype(jnp.float32) * (2.0 * math.pi / length)
    cosine = (norm * window)[:, None] * jnp.cos(phase)
    sine = -(norm * window)[:, None] * jnp.sin(phase)
    return jnp.concatenate([cosine, sine], axis=1).astype(jnp.bfloat16)

def reference(signal, offsets, kept, weights):
    table = spectral_table(kept, NFFT).astype(jnp.float32)
    scale = jnp.sqrt(weights / POINTS)

    def one_block(index):
        start = index // BLK_DEV * SEG + offsets[index]
        block = lax.dynamic_slice(signal, (start.astype(jnp.int32), jnp.int32(0)), (NFFT, POINTS))
        values = jnp.dot(table.T, block.astype(jnp.float32), preferred_element_type=jnp.float32)
        return (values * scale[None, :]).astype(jnp.bfloat16).reshape(2, K, POINTS)
    spectra = lax.map(one_block, jnp.arange(NB, dtype=jnp.int32))

    def one_freq(index):
        part = lax.dynamic_index_in_dim(spectra, index, 2, keepdims=False)
        real_part = part[:, 0, :].astype(jnp.float32)
        imag_part = part[:, 1, :].astype(jnp.float32)
        gram_re = jnp.dot(real_part, real_part.T) + jnp.dot(imag_part, imag_part.T)
        gram_im = jnp.dot(real_part, imag_part.T) - jnp.dot(imag_part, real_part.T)
        return jnp.stack([gram_re, gram_im], axis=0)
    return lax.map(one_freq, jnp.arange(K, dtype=jnp.int32))
```

```python
import math

import jax
import jax.numpy as jnp
from jax import lax
from jax.experimental import pallas as pl
from jax.experimental.pallas import tpu as pltpu
from jax.sharding import PartitionSpec as P

NFFT = 1024
ALIGN = 16
LONG = NFFT + 128


def spectral_table(kept, length):
    times = jnp.arange(length, dtype=jnp.int32)
    window = 0.5 - 0.5 * jnp.cos(times.astype(jnp.float32) * (2.0 * math.pi / length))
    norm = 1.0 / jnp.sqrt(jnp.sum(window * window))
    phase_index = kept[:, None] * times[None, :] % length
    phase = phase_index.astype(jnp.float32) * (2.0 * math.pi / length)
    cosine = (norm * window)[None, :] * jnp.cos(phase)
    sine = -(norm * window)[None, :] * jnp.sin(phase)
    both = jnp.stack([cosine, sine], axis=1).reshape(2 * kept.shape[0], length)
    return both.astype(jnp.bfloat16)


def spectra_kernel(
    offsets_ref, table_ref, scale_ref, signal_ref, out_ref, held, shifted, wide, sem
):
    rows_in = signal_ref.shape[0]
    blocks = offsets_ref.shape[0]
    rows, points = table_ref.shape[0], signal_ref.shape[1]
    dests = out_ref.shape[0]
    fetch = pltpu.make_async_copy(signal_ref, held.at[pl.ds(0, rows_in)], sem)
    fetch.start()
    held[pl.ds(rows_in, 128)] = jnp.zeros((128, points), jnp.bfloat16)
    padded = jnp.concatenate(
        [table_ref[...], jnp.zeros((rows, LONG - NFFT), jnp.float32)], axis=1
    )
    shifted[0] = padded.astype(jnp.bfloat16)

    def shift(r, carry):
        shifted[r] = pltpu.roll(padded, r, 1).astype(jnp.bfloat16)
        return carry

    lax.fori_loop(1, ALIGN, shift, 0)
    fetch.wait()
    scale = scale_ref[...]

    def one_block(n, carry):
        start = offsets_ref[n]
        base = pl.multiple_of((start // ALIGN) * ALIGN, ALIGN)
        window = held[pl.ds(base, LONG), :]
        values = jnp.dot(
            shifted[start % ALIGN], window, preferred_element_type=jnp.float32
        )
        values = values * scale
        wide[0, n, pl.ds(0, rows), :] = values[:, :128]
        wide[1, n, pl.ds(0, rows), :] = values[:, 128:]
        return carry

    lax.fori_loop(0, blocks, one_block, 0)
    flat = wide.reshape(2, blocks * wide.shape[2], 128)
    half = rows // 2

    def place(step, carry):
        for inner in range(2):
            for h in range(2):
                for c in range(2):
                    for j in range(2):
                        q = step * 2 + inner
                        row = j * half + 2 * q + c
                        picked = flat[h, pl.ds(row, blocks, stride=wide.shape[2]), :]
                        out_ref[(j * 2 + h) * (dests // 4) + q, pl.ds(c * blocks, blocks), :] = (
                            picked.astype(jnp.bfloat16)
                        )
        return carry

    lax.fori_loop(0, dests // 8, place, 0)


def gram_kernel(got_ref, out_ref):
    blks, groups, rows, lanes = got_ref.shape
    per_blk = rows // 2
    together = 8

    def some(step, total):
        pieces = []
        for i in range(together):
            p = step * together + i
            re = got_ref[:, p, :per_blk, :].reshape(blks * per_blk, lanes)
            im = got_ref[:, p, per_blk:, :].reshape(blks * per_blk, lanes)
            pieces.append(jnp.concatenate([re, im], axis=0))
        x = jnp.concatenate(pieces, axis=1)
        return total + lax.dot_general(
            x, x, (((1,), (1,)), ((), ())), preferred_element_type=jnp.float32
        )

    size = 2 * blks * per_blk
    total = lax.fori_loop(
        0, groups // together, some, jnp.zeros((size, size), jnp.float32)
    )
    nb = size // 2
    gram_re = total[:nb, :nb] + total[nb:, nb:]
    gram_im = total[:nb, nb:] - total[nb:, :nb]
    out_ref[:, 0] = gram_re.reshape(blks, per_blk, nb)
    out_ref[:, 1] = gram_im.reshape(blks, per_blk, nb)


def on_device(signal, offsets, kept, weights):
    blocks_here = offsets.shape[0]
    points_here = signal.shape[1]
    freqs = kept.shape[0]
    blks = lax.axis_size("blk")
    groups = lax.axis_size("pts")
    dests = blks * groups
    per_group = freqs // groups
    ordered = kept.reshape(groups, per_group).T.reshape(freqs)
    table = spectral_table(ordered, NFFT).astype(jnp.float32)
    scale = jnp.sqrt(weights / (points_here * groups)).reshape(1, points_here)
    vmem = pl.BlockSpec(memory_space=pltpu.VMEM)
    sent = pl.pallas_call(
        spectra_kernel,
        out_shape=jax.ShapeDtypeStruct((dests, 2 * blocks_here, 128), jnp.bfloat16),
        in_specs=[
            pl.BlockSpec(memory_space=pltpu.SMEM),
            vmem,
            vmem,
            pl.BlockSpec(memory_space=pl.ANY),
        ],
        out_specs=vmem,
        scratch_shapes=[
            pltpu.VMEM((signal.shape[0] + 128, points_here), jnp.bfloat16),
            pltpu.VMEM((ALIGN, 2 * freqs, LONG), jnp.bfloat16),
            pltpu.VMEM((2, blocks_here, 2 * freqs + 8, 128), jnp.float32),
            pltpu.SemaphoreType.DMA,
        ],
        name="spectra",
    )(offsets, table, scale, signal)
    got = lax.all_to_all(sent, ("blk", "pts"), split_axis=0, concat_axis=0, tiled=True)
    gram = pl.pallas_call(
        gram_kernel,
        out_shape=jax.ShapeDtypeStruct(
            (blks, 2, blocks_here, blks * blocks_here), jnp.float32
        ),
        in_specs=[vmem],
        out_specs=vmem,
        name="gram",
    )(got.reshape(blks, groups, 2 * blocks_here, 128))
    parts = lax.all_to_all(gram, "blk", split_axis=0, concat_axis=0, tiled=True)
    return parts[0::2] + parts[1::2]


def solution(mesh):
    placed = (P("blk", "pts"), P("blk"), P(), P("pts"))
    return jax.shard_map(
        on_device,
        mesh=mesh,
        in_specs=placed,
        out_specs=P("pts", None, "blk", None),
        check_vma=False,
    )
```

```python
import math

import jax
import jax.numpy as jnp
import numpy as np
from jax import lax
from jax.experimental import pallas as pl
from jax.experimental.pallas import tpu as pltpu
from jax.sharding import PartitionSpec as P

MESH = pl.DeviceIdType.MESH
NFFT = 1024
ALIGN = 16
LONG = NFFT + 128
PITCH = 8


def spectral_table(kept, length):
    times = jnp.arange(length, dtype=jnp.int32)
    window = 0.5 - 0.5 * np.cos(
        np.arange(length, dtype=np.float32) * np.float32(2.0 * math.pi / length)
    )
    window = window.astype(np.float32)
    norm = np.float32(1.0) / np.sqrt(np.sum(window * window, dtype=np.float32))
    gain = (norm * window).astype(np.float32)[None, :]
    phase_index = kept[:, None] * times[None, :] % length
    phase = phase_index.astype(jnp.float32) * (2.0 * math.pi / length)
    cosine = gain * jnp.cos(phase)
    sine = -gain * jnp.sin(phase)
    return cosine.astype(jnp.bfloat16), sine.astype(jnp.bfloat16)


def fused_kernel(
    offsets_ref, cos_ref, sin_ref, scale_ref, signal_ref, out_ref,
    held, padded, shifted, wide, sent, got, total, handed, final,
    load_sem, send_sem, recv_sem, hand_sem, final_sem,
):
    steps_in, _, points = signal_ref.shape
    freqs = cos_ref.shape[0]
    rows = 2 * freqs
    blocks = offsets_ref.shape[0]
    part = wide.shape[1]
    halves = blocks // part

    blk = lax.axis_index("blk")
    pts = lax.axis_index("pts")
    core = lax.rem(pts, 2)
    x = lax.rem(pts // 2, 4)
    zh = lax.rem(pts // 8, 2)
    y = pts // 16

    def device(b, zh_, y_, x_, c_):
        return (b, ((y_ * 2 + zh_) * 4 + x_) * 2 + c_)

    def slot(b, y_, x_, c_):
        return y_ * 32 + (x_ * 2 + c_) * 4 + b

    def peer(dy, inner):
        turn = inner // 4
        way = lax.rem(inner, 4)
        b2 = jnp.bitwise_xor(blk, jnp.where(way == 0, 2, jnp.where(way == 1, 1, jnp.where(way == 2, 3, 0))))
        y2 = lax.rem(y + dy, 4)
        x2 = lax.rem(x + turn // 2, 4)
        c2 = lax.rem(core + turn, 2)
        return b2, y2, x2, c2

    mine = slot(blk, y, x, core)

    fetch = pltpu.make_async_copy(signal_ref, held.at[pl.ds(0, steps_in)], load_sem)
    fetch.start()

    barrier = pltpu.get_barrier_semaphore()

    def greet(i, carry):
        b2, y2, x2, c2 = peer(i // 32, lax.rem(i, 32))

        @pl.when(i != 3)
        def _():
            pl.semaphore_signal(
                barrier, inc=1, device_id=device(b2, zh, y2, x2, c2), device_id_type=MESH
            )

        return carry

    lax.fori_loop(0, 128, greet, 0)

    def greet_far(b2, carry):
        pl.semaphore_signal(
            barrier, inc=1, device_id=device(b2, 1 - zh, y, x, core), device_id_type=MESH
        )
        return carry

    lax.fori_loop(0, 4, greet_far, 0)

    spare = held.shape[0] - steps_in
    held[pl.ds(steps_in, spare)] = jnp.zeros((spare, ALIGN, points), jnp.bfloat16)
    padded[pl.ds(0, freqs), pl.ds(0, NFFT)] = cos_ref[...].astype(jnp.float32)
    padded[pl.ds(freqs, freqs), pl.ds(0, NFFT)] = sin_ref[...].astype(jnp.float32)
    padded[:, pl.ds(NFFT, LONG - NFFT)] = jnp.zeros((rows, LONG - NFFT), jnp.float32)

    def shift(step, carry):
        r = step // 8
        some = pl.ds(pl.multiple_of(lax.rem(step, 8) * (rows // 8), rows // 8), rows // 8)
        shifted[r, some, :] = pltpu.roll(padded[some, :], r, 1).astype(jnp.bfloat16)
        return carry

    lax.fori_loop(0, ALIGN * 8, shift, 0)
    scale = scale_ref[...]
    fetch.wait()

    for s in range(halves):

        def one_block(i, carry):
            for u in range(2):
                n = i * 2 + u
                start = offsets_ref[s * part + n]
                window = held[pl.ds(lax.div(start, ALIGN), LONG // ALIGN)]
                values = jnp.dot(
                    shifted[lax.rem(start, ALIGN)],
                    window.reshape(LONG, points),
                    preferred_element_type=jnp.float32,
                )
                values = values * scale
                wide[0, n, pl.ds(0, rows), :] = values[:, :128]
                wide[1, n, pl.ds(0, rows), :] = values[:, 128:]
            return carry

        lax.fori_loop(0, part // 2, one_block, 0)
        flat = wide.reshape(2, part * wide.shape[2], 128)

        def place(step, carry):
            for u in range(4):
                i = step * 4 + u
                b_ = u
                c_ = lax.rem(i // 4, 2)
                x_ = lax.rem(i // 8, 4)
                y_ = i // 32
                k = ((y_ * 2 + b_ // 2) * 4 + x_) * 4 + c_ * 2 + b_ % 2
                for h in range(2):
                    for ri in range(2):
                        picked = flat[h, pl.ds(ri * freqs + k, part, stride=wide.shape[2]), :]
                        sent[s, i, h, pl.ds(ri * part, part), :] = picked.astype(jnp.bfloat16)
            return carry

        lax.fori_loop(0, 32, place, 0)
        got[s, mine] = sent[s, mine]
        if s == 0:
            pl.semaphore_wait(barrier, 131)

        for dy in range(4):

            def send(inner, carry):
                b2, y2, x2, c2 = peer(dy, inner)

                @pl.when(jnp.logical_or(inner != 3, dy != 0))
                def _():
                    pltpu.make_async_remote_copy(
                        src_ref=sent.at[s, slot(b2, y2, x2, c2)],
                        dst_ref=got.at[s, mine],
                        send_sem=send_sem.at[s],
                        recv_sem=recv_sem.at[0 if s == 0 else 1 + dy],
                        device_id=device(b2, zh, y2, x2, c2),
                        device_id_type=MESH,
                    ).start()

                return carry

            lax.fori_loop(0, 32, send, 0)

    def arrived(s, lo, count, sem):
        some = got.at[s, pl.ds(lo, count)]
        pltpu.make_async_copy(some, some, sem).wait()

    size = 2 * 4 * blocks
    total[...] = jnp.zeros((size, size), jnp.float32)
    arrived(0, 0, 127, recv_sem.at[0])
    for dy in range(4):
        y_from = lax.rem(y - dy + 4, 4)
        if dy == 0:
            arrived(1, 0, 31, recv_sem.at[1])
        else:
            arrived(1, pl.multiple_of(y_from * 32, 32), 32, recv_sem.at[1 + dy])

        def some_points(step, carry):
            pieces = []
            for u in range(4):
                place_ = y_from * 32 + (step * 4 + u) * 4
                for h in range(2):
                    stack = []
                    for ri in range(2):
                        for b_ in range(4):
                            for s in range(halves):
                                stack.append(got[s, place_ + b_, h, pl.ds(ri * part, part), :])
                    pieces.append(jnp.concatenate(stack, axis=0))
            block = jnp.concatenate(pieces, axis=1)
            total[...] += lax.dot_general(
                block, block, (((1,), (1,)), ((), ())), preferred_element_type=jnp.float32
            )
            return carry

        lax.fori_loop(0, 2, some_points, 0)

    nb = size // 2
    gram_re = total[pl.ds(0, nb), pl.ds(0, nb)] + total[pl.ds(nb, nb), pl.ds(nb, nb)]
    gram_im = total[pl.ds(0, nb), pl.ds(nb, nb)] - total[pl.ds(nb, nb), pl.ds(0, nb)]
    handed[:, 0] = gram_re.reshape(4, blocks, nb)
    handed[:, 1] = gram_im.reshape(4, blocks, nb)

    goal = blk // 2
    here = zh * 2 + lax.rem(blk, 2)
    own = goal == zh

    def hand(b2, carry):
        @pl.when(jnp.logical_or(jnp.logical_not(own), b2 != blk))
        def _():
            pltpu.make_async_remote_copy(
                src_ref=handed.at[b2],
                dst_ref=final.at[here],
                send_sem=hand_sem,
                recv_sem=final_sem,
                device_id=device(b2, goal, y, x, core),
                device_id_type=MESH,
            ).start()

        return carry

    lax.fori_loop(0, 4, hand, 0)

    @pl.when(own)
    def _():
        final[here] = handed[blk]
        three = handed.at[pl.ds(0, 3)]
        pltpu.make_async_copy(three, three, hand_sem).wait()
        three = final.at[pl.ds(0, 3)]
        pltpu.make_async_copy(three, three, final_sem).wait()

    @pl.when(jnp.logical_not(own))
    def _():
        pltpu.make_async_copy(handed, handed, hand_sem).wait()
        pltpu.make_async_copy(final, final, final_sem).wait()

    out_ref[...] = final[pl.ds(0, 2)] + final[pl.ds(2, 2)]
    for s in range(halves):
        some = sent.at[s, pl.ds(0, 127)]
        pltpu.make_async_copy(some, some, send_sem.at[s]).wait()


def on_device(signal, offsets, kept, weights):
    blocks = offsets.shape[0]
    points = signal.shape[1]
    freqs = kept.shape[0]
    groups = lax.axis_size("pts")
    cosine, sine = spectral_table(kept, NFFT)
    scale = jnp.sqrt(weights / (points * groups)).reshape(1, points)
    vmem = pl.BlockSpec(memory_space=pltpu.VMEM)
    part = blocks // 2
    size = 8 * blocks
    return pl.pallas_call(
        fused_kernel,
        out_shape=jax.ShapeDtypeStruct((2, 2, blocks, 4 * blocks), jnp.float32),
        in_specs=[
            pl.BlockSpec(memory_space=pltpu.SMEM),
            vmem,
            vmem,
            vmem,
            pl.BlockSpec(memory_space=pl.ANY),
        ],
        out_specs=vmem,
        scratch_shapes=[
            pltpu.VMEM(((signal.shape[0] + LONG - NFFT) // ALIGN, ALIGN, points), jnp.bfloat16),
            pltpu.VMEM((2 * freqs, LONG), jnp.float32),
            pltpu.VMEM((ALIGN, 2 * freqs, LONG), jnp.bfloat16),
            pltpu.VMEM((2, part, 2 * freqs + PITCH, 128), jnp.float32),
            pltpu.VMEM((2, 128, 2, 2 * part, 128), jnp.bfloat16),
            pltpu.VMEM((2, 128, 2, 2 * part, 128), jnp.bfloat16),
            pltpu.VMEM((size, size), jnp.float32),
            pltpu.VMEM((4, 2, blocks, 4 * blocks), jnp.float32),
            pltpu.VMEM((4, 2, blocks, 4 * blocks), jnp.float32),
            pltpu.SemaphoreType.DMA,
            pltpu.SemaphoreType.DMA((2,)),
            pltpu.SemaphoreType.DMA((5,)),
            pltpu.SemaphoreType.DMA,
            pltpu.SemaphoreType.DMA,
        ],
        compiler_params=pltpu.CompilerParams(collective_id=0, has_side_effects=True),
        name="spod",
    )(offsets, cosine, sine, scale, signal.reshape(-1, ALIGN, points))


def solution(mesh):
    placed = (P("blk", "pts"), P("blk"), P(), P("pts"))
    return jax.shard_map(
        on_device,
        mesh=mesh,
        in_specs=placed,
        out_specs=P("pts", None, "blk", None),
        check_vma=False,
    )
```
